32 devices in a mesh: fsdp: 8 (over y, x, core), model: 4 (over z).
Axes of the slice: x: 2, y: 2, z: 4, core: 2. Of those that a mesh axis runs over, the one named last changes fastest.
Arguments:
- w_query: float32 [4096, 4096], P('fsdp', 'model'), may hold values from -0.125 to 0.125
- first_query: float32 [4096, 4096], P('fsdp', 'model'), may hold values from -0.09375 to 0.09375
- second_query: float32 [4096, 4096], P('fsdp', 'model'), may hold values from -0.09375 to 0.09375
- w_key: float32 [4096, 4096], P('fsdp', 'model'), may hold values from -0.125 to 0.125
- first_key: float32 [4096, 4096], P('fsdp', 'model'), may hold values from -0.09375 to 0.09375
- second_key: float32 [4096, 4096], P('fsdp', 'model'), may hold values from -0.09375 to 0.09375
- w_value: float32 [4096, 4096], P('fsdp', 'model'), may hold values from -0.125 to 0.125
- first_value: float32 [4096, 4096], P('fsdp', 'model'), may hold values from -0.09375 to 0.09375
- second_value: float32 [4096, 4096], P('fsdp', 'model'), may hold values from -0.09375 to 0.09375
- norm_gain: float32 [4096], P('fsdp'), may hold values from 0.25 to 1.75
Outputs:
- ready_query: bfloat16 [4096, 4096], P(None, 'model')
- ready_key: bfloat16 [4096, 4096], P(None, 'model')
- ready_value: bfloat16 [4096, 4096], P(None, 'model')
- factor_query: float32 [4096], P('model')
- factor_key: float32 [4096], P('model')
- factor_value: float32 [4096], P('model')
The draws below stay inside these ranges and needn't reach their ends.
All inputs are finite; a program needn't handle non-finite values. Where the reference program divides by a largest or mean magnitude, that divisor is 1e-20 or more.
Results may differ from the reference program's by a relative error of at most 0.001.
Values may be sent and summed in bfloat16 or wider, within the bound.
A program may use at most 128 MiB of HBM per device.

```python
import jax
import jax.numpy as jnp

D_MODEL = 4096
Q_DIM = 4096
KV_DIM = 4096


def strengthened(values, own_key, source, target, shards_of, factor):
    def block_of(axis_at):
        return (jnp.arange(values.shape[axis_at]) // (values.shape[axis_at] // shards_of)).reshape((-1,) + (1,) * (values.ndim - 1 - axis_at))

    one_side = jax.random.permutation(own_key, shards_of)[block_of(target)]
    far = (block_of(target) + shards_of // 2) % shards_of
    return jnp.where((block_of(source) == one_side) | (block_of(source) == far), factor * values, values)


def levels(key, extent, cuts, low, top_value):
    gain, own = 1.0, jax.random.fold_in(key, 6)
    for position, parts in cuts:
        heights = jnp.exp(jax.random.uniform(jax.random.fold_in(own, position), (parts,), jnp.float32, low / len(cuts), top_value / len(cuts)))
        gain = gain * jnp.repeat(heights, extent[position] // parts).reshape([-1 if axis == position else 1 for axis in range(len(extent))])
    return gain


def centred(own_key, shape, deviation, most, split=(), kind=jnp.bfloat16):
    values = deviation * jax.random.normal(own_key, shape, jnp.float32)
    if split:
        values = values * levels(own_key, shape, split, -0.22, 0.18)
    return jnp.clip(values, -most, most).astype(kind)


def gaussian_with(key, extent, scale, most, pieces, heavy, kind=jnp.bfloat16):
    drawn = scale * jax.random.normal(key, extent, jnp.float32)
    if pieces:
        drawn = drawn * levels(key, extent, pieces, -0.22, 0.18)
    return jnp.clip(strengthened(drawn, jax.random.fold_in(key, 3), *heavy), -most, most).astype(kind)


def setup_inputs(seed: int = 0) -> dict:
    key_of = jax.random.split(jax.random.key(seed), 11)
    return {
        "w_query": gaussian_with(key_of[0], (D_MODEL, Q_DIM), D_MODEL ** -0.5, 0.125, ((0, 8), (1, 4)), (0, 1, 8, 2.0), jnp.float32),
        "first_query": centred(key_of[1], (D_MODEL, Q_DIM), D_MODEL ** -0.5, 0.09375, ((0, 8), (1, 4)), jnp.float32),
        "second_query": centred(key_of[2], (D_MODEL, Q_DIM), D_MODEL ** -0.5, 0.09375, ((0, 8), (1, 4)), jnp.float32),
        "w_key": gaussian_with(key_of[3], (D_MODEL, KV_DIM), D_MODEL ** -0.5, 0.125, ((0, 8), (1, 4)), (0, 1, 8, 2.0), jnp.float32),
        "first_key": centred(key_of[4], (D_MODEL, KV_DIM), D_MODEL ** -0.5, 0.09375, ((0, 8), (1, 4)), jnp.float32),
        "second_key": centred(key_of[5], (D_MODEL, KV_DIM), D_MODEL ** -0.5, 0.09375, ((0, 8), (1, 4)), jnp.float32),
        "w_value": gaussian_with(key_of[6], (D_MODEL, KV_DIM), D_MODEL ** -0.5, 0.125, ((0, 8), (1, 4)), (0, 1, 8, 2.0), jnp.float32),
        "first_value": centred(key_of[7], (D_MODEL, KV_DIM), D_MODEL ** -0.5, 0.09375, ((0, 8), (1, 4)), jnp.float32),
        "second_value": centred(key_of[8], (D_MODEL, KV_DIM), D_MODEL ** -0.5, 0.09375, ((0, 8), (1, 4)), jnp.float32),
        "norm_gain": jnp.clip(1.0 + 0.15 * jax.random.normal(key_of[9], (D_MODEL,), jnp.float32), 0.25, 1.75),
    }


learn_rate = 0.2
hold_rate = 0.9


def reference(w_query, first_query, second_query, w_key, first_key, second_key, w_value, first_value, second_value, norm_gain):
    hold_query = hold_rate * first_query + second_query
    latest_query = w_query - learn_rate * hold_query
    hold_key = hold_rate * first_key + second_key
    latest_key = w_key - learn_rate * hold_key
    hold_value = hold_rate * first_value + second_value
    latest_value = w_value - learn_rate * hold_value
    latest_gained_query = latest_query * norm_gain[:, None]
    latest_gained_key = latest_key * norm_gain[:, None]
    latest_gained_value = latest_value * norm_gain[:, None]
    factor_query = jnp.sum(jnp.abs(latest_gained_query), axis=0) / D_MODEL
    ready_query = (latest_gained_query / factor_query).astype(jnp.bfloat16)
    factor_key = jnp.sum(jnp.abs(latest_gained_key), axis=0) / D_MODEL
    ready_key = (latest_gained_key / factor_key).astype(jnp.bfloat16)
    factor_value = jnp.sum(jnp.abs(latest_gained_value), axis=0) / D_MODEL
    ready_value = (latest_gained_value / factor_value).astype(jnp.bfloat16)
    return ready_query, ready_key, ready_value, factor_query, factor_key, factor_value
```

```python
import functools
import math

import jax
import jax.numpy as jnp
from jax import lax
from jax.experimental import pallas as pl
from jax.experimental.pallas import tpu as pltpu
from jax.sharding import PartitionSpec as P

learn_rate = 0.2
hold_rate = 0.9
MESH = pl.DeviceIdType.MESH
UNITS = 2
STEP = 32


def plain(
    w_query,
    first_query,
    second_query,
    w_key,
    first_key,
    second_key,
    w_value,
    first_value,
    second_value,
    norm_gain,
    rows,
):
    gained = []
    for w, first, second in (
        (w_query, first_query, second_query),
        (w_key, first_key, second_key),
        (w_value, first_value, second_value),
    ):
        hold = hold_rate * first + second
        gained.append((w - learn_rate * hold) * norm_gain[:, None])
    totals = lax.psum(tuple(jnp.sum(jnp.abs(g), axis=0) for g in gained), "fsdp")
    factors = tuple(t / rows for t in totals)
    ready = tuple(
        lax.all_gather(
            (g / f).astype(jnp.bfloat16), "fsdp", axis=0, tiled=True
        )
        for g, f in zip(gained, factors)
    )
    return ready + factors


def gather_kernel(total_rows, *refs):
    ins, gain_ref = refs[:9], refs[9]
    outs, factor_ref = refs[10:13], refs[13]
    (
        w_buf, first_buf, second_buf, gain_buf, mine, parts,
        load_sem, sum_send, sum_recv, x_recv, y_recv, diag_recv,
        chip_recv, send_sem,
    ) = refs[14:]
    bufs = (w_buf, first_buf, second_buf)
    rows, cols = w_buf.shape[1:]
    width = cols // UNITS
    half = rows // 2

    me = lax.axis_index("fsdp")
    core = me % 2
    x = (me // 2) % 2
    y = me // 4
    partner = me + 1 - 2 * core
    x_near = me + 2 - 4 * x
    y_near = me + 4 - 8 * y
    diag = x_near + 4 - 8 * y
    peers = [
        partner, x_near, y_near, diag,
        x_near + 1 - 2 * core, y_near + 1 - 2 * core, diag + 1 - 2 * core,
    ]

    units = [(m, c) for m in range(3) for c in range(UNITS)]
    loads = []
    for u, (m, c) in enumerate(units):
        at = pl.ds(c * width, width)
        loads.append([
            pltpu.make_async_copy(
                ins[3 * m + k].at[:, at], bufs[k].at[m, :, at], load_sem.at[u, k]
            )
            for k in range(3)
        ])
    for group in loads:
        for copy in group:
            copy.start()

    barrier = pltpu.get_barrier_semaphore()
    for peer in peers:
        pl.semaphore_signal(
            barrier, inc=1, device_id={"fsdp": peer}, device_id_type=MESH
        )

    for k in range(rows // 128):
        line = gain_ref[:, pl.ds(k * 128, 128)]
        gain_buf[pl.ds(k * 128, 128), :] = jnp.broadcast_to(line, (128, 128)).T

    def sums(u):
        m, c = units[u]
        for copy in loads[u]:
            copy.wait()
        tiles = width // 128

        def body(i, acc):
            at = pl.ds(pl.multiple_of(i * STEP, STEP), STEP)
            gain = gain_buf[at, :]
            new = []
            for t in range(tiles):
                lanes = pl.ds(c * width + t * 128, 128)
                hold = hold_rate * first_buf[m, at, lanes] + second_buf[m, at, lanes]
                gained = (w_buf[m, at, lanes] - learn_rate * hold) * gain
                w_buf[m, at, lanes] = gained
                size = jnp.abs(gained)
                new.append(
                    acc[t] + jnp.sum(size.reshape(STEP // 8, 8, 128), axis=0)
                )
            return tuple(new)

        acc = lax.fori_loop(
            0, rows // STEP, body,
            tuple(jnp.zeros((8, 128), jnp.float32) for _ in range(tiles)),
        )
        for t in range(tiles):
            mine[u, :, pl.ds(t * 128, 128)] = jnp.sum(acc[t], axis=0, keepdims=True)

    def sum_copy(u, slot, peer):
        return pltpu.make_async_remote_copy(
            src_ref=mine.at[u],
            dst_ref=parts.at[u, slot],
            send_sem=sum_send.at[u, slot],
            recv_sem=sum_recv.at[u, slot],
            device_id={"fsdp": peer},
            device_id_type=MESH,
        )

    def send_sums(u):
        for slot, peer in enumerate(peers):
            sum_copy(u, slot, peer).start()

    def block(m, c, owner, first, count):
        at = pl.ds(pl.multiple_of(owner * rows + first, 16), count)
        return outs[m].at[at, pl.ds(c * width, width)]

    def send(m, ref, recv_sem, peer):
        pltpu.make_async_remote_copy(
            src_ref=ref, dst_ref=ref, send_sem=send_sem.at[m], recv_sem=recv_sem,
            device_id={"fsdp": peer}, device_id_type=MESH,
        ).start()

    def arrived(ref, recv_sem):
        pltpu.make_async_remote_copy(
            src_ref=ref, dst_ref=ref, send_sem=send_sem.at[0], recv_sem=recv_sem,
            device_id={"fsdp": partner}, device_id_type=MESH,
        ).wait_recv()

    def finish(u):
        m, c = units[u]
        for slot, peer in enumerate(peers):
            sum_copy(u, slot, peer).wait_recv()
        total = mine[u]
        for slot in range(7):
            total = total + parts[u, slot]
        factor = total / total_rows
        factor_ref[pl.ds(m, 1), pl.ds(c * width, width)] = factor
        scale = jnp.broadcast_to(1.0 / factor, (16, width))

        def body(i, carry):
            for k in range(STEP // 16):
                at = pl.multiple_of(i * STEP + k * 16, 16)
                tile = w_buf[m, pl.ds(at, 16), pl.ds(c * width, width)] * scale
                outs[m][
                    pl.ds(pl.multiple_of(me * rows + at, 16), 16),
                    pl.ds(c * width, width),
                ] = tile.astype(jnp.bfloat16)
            return carry

        for h in range(2):
            lo = h * half // STEP
            lax.fori_loop(lo, lo + half // STEP, body, 0)
            ref = block(m, c, me, h * half, half)
            send(m, ref, x_recv.at[u, h], x_near)
            send(m, ref, y_recv.at[u, h], y_near)
        send(m, block(m, c, me, 0, rows), chip_recv.at[m], partner)

    count = len(units)
    for u in range(count):
        sums(u)
        if u == 0:
            pl.semaphore_wait(barrier, 7)
        send_sums(u)
        if u >= 1:
            finish(u - 1)
    finish(count - 1)

    for u, (m, c) in enumerate(units):
        for h in range(2):
            ref = block(m, c, x_near, h * half, half)
            arrived(ref, x_recv.at[u, h])
            if h == 0:
                send(m, ref, diag_recv.at[u, 0], y_near)
            send(m, ref, chip_recv.at[m], partner)
            ref = block(m, c, y_near, h * half, half)
            arrived(ref, y_recv.at[u, h])
            if h == 1:
                send(m, ref, diag_recv.at[u, 1], x_near)
            send(m, ref, chip_recv.at[m], partner)
    for u, (m, c) in enumerate(units):
        for h in range(2):
            ref = block(m, c, diag, h * half, half)
            arrived(ref, diag_recv.at[u, h])
            send(m, ref, chip_recv.at[m], partner)

    for m in range(3):
        taken = outs[m].at[pl.ds(0, 4 * rows), :]
        sent = outs[m].at[pl.ds(0, 7 * rows), :]
        arrived(taken, chip_recv.at[m])
        pltpu.make_async_remote_copy(
            src_ref=sent, dst_ref=sent, send_sem=send_sem.at[m],
            recv_sem=chip_recv.at[m], device_id={"fsdp": partner},
            device_id_type=MESH,
        ).wait_send()
    for u in range(count):
        for slot, peer in enumerate(peers):
            sum_copy(u, slot, peer).wait_send()


def write_kernel(a, b, c, factor, out_a, out_b, out_c, fa, fb, fc, sem):
    copies = []
    for k, (src, dst) in enumerate(((a, out_a), (b, out_b), (c, out_c))):
        rows = src.shape[0] // 4
        for p in range(4):
            at = pl.ds(p * rows, rows)
            copies.append(
                pltpu.make_async_copy(src.at[at, :], dst.at[at, :], sem.at[k, p])
            )
    for copy in copies:
        copy.start()
    for m, out in enumerate((fa, fb, fc)):
        out[...] = factor[m, :]
    for copy in copies:
        copy.wait()


def ringed(*args, total_rows):
    rows, cols = args[0].shape
    count = 3 * UNITS
    width = cols // UNITS
    big = (8 * rows, cols)
    vmem = pl.BlockSpec(memory_space=pltpu.VMEM)
    hbm = pl.BlockSpec(memory_space=pltpu.HBM)
    buf = pltpu.VMEM((3, rows, cols), jnp.float32)
    dma = pltpu.SemaphoreType.DMA
    *gathered, factor = pl.pallas_call(
        functools.partial(gather_kernel, total_rows),
        out_shape=[pltpu.VMEM(big, jnp.bfloat16)] * 3
        + [pltpu.VMEM((3, cols), jnp.float32)],
        in_specs=[hbm] * 9 + [vmem],
        out_specs=[vmem] * 4,
        scratch_shapes=[
            buf, buf, buf,
            pltpu.VMEM((rows, 128), jnp.float32),
            pltpu.VMEM((count, 1, width), jnp.float32),
            pltpu.VMEM((count, 7, 1, width), jnp.float32),
            dma((count, 3)),
            dma((count, 7)), dma((count, 7)),
            dma((count, 2)), dma((count, 2)), dma((count, 2)),
            dma((3,)), dma((3,)),
        ],
        compiler_params=pltpu.CompilerParams(
            collective_id=0, has_side_effects=True,
            vmem_limit_bytes=24 * 2**20,
        ),
        name="gather",
    )(*args[:9], args[9].reshape(1, rows))
    ready = jax.ShapeDtypeStruct(big, jnp.bfloat16)
    line = jax.ShapeDtypeStruct((cols,), jnp.float32)
    return pl.pallas_call(
        write_kernel,
        out_shape=[ready] * 3 + [line] * 3,
        in_specs=[vmem] * 4,
        out_specs=[hbm] * 3 + [vmem] * 3,
        scratch_shapes=[dma((3, 4))],
        compiler_params=pltpu.CompilerParams(vmem_limit_bytes=2**20),
        name="write",
    )(*gathered, factor)


def on_device(*args, devices):
    rows, cols = args[0].shape
    total_rows = devices * rows
    fits = rows * cols * (36 + 48) <= 48 * 2**20
    if devices == 8 and rows % 128 == 0 and cols % (128 * UNITS) == 0 and fits:
        return tuple(ringed(*args, total_rows=total_rows))
    return plain(*args, rows=total_rows)


def solution(mesh):
    return jax.shard_map(
        functools.partial(on_device, devices=mesh.shape["fsdp"]),
        mesh=mesh,
        in_specs=(P("fsdp", "model"),) * 9 + (P("fsdp"),),
        out_specs=(P(None, "model"),) * 3 + (P("model"),) * 3,
        check_vma=False,
    )
```

```python
import functools
import math

import jax
import jax.numpy as jnp
from jax import lax
from jax.experimental import pallas as pl
from jax.experimental.pallas import tpu as pltpu
from jax.sharding import PartitionSpec as P

learn_rate = 0.2
hold_rate = 0.9
MESH = pl.DeviceIdType.MESH
UNITS = 4
PARTS = ((1, 1, 2), (2, 2), (2, 1, 1))
STEP = 32
AHEAD = 2
VMEM_BYTES = 67_043_328


def plain(
    w_query,
    first_query,
    second_query,
    w_key,
    first_key,
    second_key,
    w_value,
    first_value,
    second_value,
    norm_gain,
    rows,
):
    gained = []
    for w, first, second in (
        (w_query, first_query, second_query),
        (w_key, first_key, second_key),
        (w_value, first_value, second_value),
    ):
        hold = hold_rate * first + second
        gained.append((w - learn_rate * hold) * norm_gain[:, None])
    totals = lax.psum(tuple(jnp.sum(jnp.abs(g), axis=0) for g in gained), "fsdp")
    factors = tuple(t / rows for t in totals)
    ready = tuple(
        lax.all_gather(
            (g / f).astype(jnp.bfloat16), "fsdp", axis=0, tiled=True
        )
        for g, f in zip(gained, factors)
    )
    return ready + factors


def units_of(cols):
    units = []
    for m, sizes in enumerate(PARTS):
        first = 0
        for size in sizes:
            units.append((m, first, size * cols // UNITS))
            first += size * cols // UNITS
    return units


def gather_kernel(total_rows, *refs):
    ins, gain_ref = refs[:9], refs[9]
    outs, factor_ref = refs[10:13], refs[13]
    (
        w_buf, first_buf, second_buf, gain_line, gain_buf, mine, parts,
        load_sem, gain_sem, sum_send, sum_recv, x_recv, y_recv, diag_recv,
        chip_recv, send_sem,
    ) = refs[14:]
    bufs = (w_buf, first_buf, second_buf)
    rows, cols = w_buf.shape[1:]
    half = rows // 2

    me = lax.axis_index("fsdp")
    core = me % 2
    x = (me // 2) % 2
    y = me // 4
    partner = me + 1 - 2 * core
    x_near = me + 2 - 4 * x
    y_near = me + 4 - 8 * y
    diag = x_near + 4 - 8 * y
    peers = [
        partner, x_near, y_near, diag,
        x_near + 1 - 2 * core, y_near + 1 - 2 * core, diag + 1 - 2 * core,
    ]

    units = units_of(cols)
    loads = []
    for u, (m, c, width) in enumerate(units):
        at = pl.ds(c, width)
        loads.append([
            pltpu.make_async_copy(
                ins[3 * m + k].at[:, at], bufs[k].at[m, :, at], load_sem.at[u, k]
            )
            for k in range(3)
        ])

    def load(u):
        if u < len(units):
            for copy in loads[u]:
                copy.start()

    gain_copy = pltpu.make_async_copy(gain_ref, gain_line, gain_sem)
    gain_copy.start()
    for u in range(AHEAD):
        load(u)

    barrier = pltpu.get_barrier_semaphore()
    for peer in peers:
        pl.semaphore_signal(
            barrier, inc=1, device_id={"fsdp": peer}, device_id_type=MESH
        )

    gain_copy.wait()
    for k in range(rows // 128):
        line = gain_line[:, pl.ds(k * 128, 128)]
        gain_buf[pl.ds(k * 128, 128), :] = jnp.broadcast_to(line, (128, 128)).T

    def sums(u):
        m, c, width = units[u]
        for copy in loads[u]:
            copy.wait()
        load(u + AHEAD)
        tiles = width // 128

        def body(i, acc):
            at = pl.ds(pl.multiple_of(i * STEP, STEP), STEP)
            gain = gain_buf[at, :]
            new = []
            for t in range(tiles):
                lanes = pl.ds(c + t * 128, 128)
                hold = hold_rate * first_buf[m, at, lanes] + second_buf[m, at, lanes]
                gained = (w_buf[m, at, lanes] - learn_rate * hold) * gain
                w_buf[m, at, lanes] = gained
                size = jnp.abs(gained)
                new.append(
                    acc[t] + jnp.sum(size.reshape(STEP // 8, 8, 128), axis=0)
                )
            return tuple(new)

        acc = lax.fori_loop(
            0, rows // STEP, body,
            tuple(jnp.zeros((8, 128), jnp.float32) for _ in range(tiles)),
        )
        for t in range(tiles):
            mine[u, :, pl.ds(t * 128, 128)] = jnp.sum(acc[t], axis=0, keepdims=True)

    def sum_copy(u, slot, peer):
        return pltpu.make_async_remote_copy(
            src_ref=mine.at[u, :, pl.ds(0, units[u][2])],
            dst_ref=parts.at[u, slot, :, pl.ds(0, units[u][2])],
            send_sem=sum_send.at[u, slot],
            recv_sem=sum_recv.at[u, slot],
            device_id={"fsdp": peer},
            device_id_type=MESH,
        )

    def send_sums(u):
        for slot, peer in enumerate(peers):
            sum_copy(u, slot, peer).start()

    def block(u, owner, first, count):
        m, c, width = units[u]
        at = pl.ds(pl.multiple_of(owner * rows + first, 16), count)
        return outs[m].at[at, pl.ds(c, width)]

    def send(m, ref, recv_sem, peer):
        pltpu.make_async_remote_copy(
            src_ref=ref, dst_ref=ref, send_sem=send_sem.at[m], recv_sem=recv_sem,
            device_id={"fsdp": peer}, device_id_type=MESH,
        ).start()

    def arrived(ref, recv_sem):
        pltpu.make_async_remote_copy(
            src_ref=ref, dst_ref=ref, send_sem=send_sem.at[0], recv_sem=recv_sem,
            device_id={"fsdp": partner}, device_id_type=MESH,
        ).wait_recv()

    def finish(u):
        m, c, width = units[u]
        for slot, peer in enumerate(peers):
            sum_copy(u, slot, peer).wait_recv()
        total = mine[u, :, pl.ds(0, width)]
        for slot in range(7):
            total = total + parts[u, slot, :, pl.ds(0, width)]
        factor = total / total_rows
        factor_ref[pl.ds(m, 1), pl.ds(c, width)] = factor
        scale = jnp.broadcast_to(1.0 / factor, (16, width))

        def body(i, carry):
            for k in range(STEP // 16):
                at = pl.multiple_of(i * STEP + k * 16, 16)
                tile = w_buf[m, pl.ds(at, 16), pl.ds(c, width)] * scale
                outs[m][
                    pl.ds(pl.multiple_of(me * rows + at, 16), 16),
                    pl.ds(c, width),
                ] = tile.astype(jnp.bfloat16)
            return carry

        for h in range(2):
            lo = h * half // STEP
            lax.fori_loop(lo, lo + half // STEP, body, 0)
            ref = block(u, me, h * half, half)
            send(m, ref, x_recv.at[u, h], x_near)
            send(m, ref, y_recv.at[u, h], y_near)
        send(m, block(u, me, 0, rows), chip_recv.at[m], partner)

    count = len(units)
    for u in range(count):
        sums(u)
        if u == 0:
            pl.semaphore_wait(barrier, 7)
        send_sums(u)
        if u >= 1:
            finish(u - 1)
    finish(count - 1)

    for u, (m, _, _) in enumerate(units):
        for h in range(2):
            ref = block(u, x_near, h * half, half)
            arrived(ref, x_recv.at[u, h])
            if h == 0:
                send(m, ref, diag_recv.at[u, 0], y_near)
            send(m, ref, chip_recv.at[m], partner)
            ref = block(u, y_near, h * half, half)
            arrived(ref, y_recv.at[u, h])
            if h == 1:
                send(m, ref, diag_recv.at[u, 1], x_near)
            send(m, ref, chip_recv.at[m], partner)
    for u, (m, _, _) in enumerate(units):
        for h in range(2):
            ref = block(u, diag, h * half, half)
            arrived(ref, diag_recv.at[u, h])
            send(m, ref, chip_recv.at[m], partner)

    for m in range(3):
        taken = outs[m].at[pl.ds(0, 4 * rows), :]
        sent = outs[m].at[pl.ds(0, 7 * rows), :]
        arrived(taken, chip_recv.at[m])
        pltpu.make_async_remote_copy(
            src_ref=sent, dst_ref=sent, send_sem=send_sem.at[m],
            recv_sem=chip_recv.at[m], device_id={"fsdp": partner},
            device_id_type=MESH,
        ).wait_send()
    for u in range(count):
        for slot, peer in enumerate(peers):
            sum_copy(u, slot, peer).wait_send()


def write_kernel(a, b, c, factor, out_a, out_b, out_c, fa, fb, fc, sem):
    copies = []
    for k, (src, dst) in enumerate(((a, out_a), (b, out_b), (c, out_c))):
        rows = src.shape[0] // 4
        for p in range(4):
            at = pl.ds(p * rows, rows)
            copies.append(
                pltpu.make_async_copy(src.at[at, :], dst.at[at, :], sem.at[k, p])
            )
    for copy in copies:
        copy.start()
    for m, out in enumerate((fa, fb, fc)):
        out[...] = factor[m, :]
    for copy in copies:
        copy.wait()


def ringed(*args, total_rows):
    rows, cols = args[0].shape
    units = units_of(cols)
    count = len(units)
    width = max(unit[2] for unit in units)
    big = (8 * rows, cols)
    vmem = pl.BlockSpec(memory_space=pltpu.VMEM)
    hbm = pl.BlockSpec(memory_space=pltpu.HBM)
    buf = pltpu.VMEM((3, rows, cols), jnp.float32)
    dma = pltpu.SemaphoreType.DMA
    *gathered, factor = pl.pallas_call(
        functools.partial(gather_kernel, total_rows),
        out_shape=[pltpu.VMEM(big, jnp.bfloat16)] * 3
        + [pltpu.VMEM((3, cols), jnp.float32)],
        in_specs=[hbm] * 10,
        out_specs=[vmem] * 4,
        scratch_shapes=[
            buf, buf, buf,
            pltpu.VMEM((1, rows), jnp.float32),
            pltpu.VMEM((rows, 128), jnp.float32),
            pltpu.VMEM((count, 1, width), jnp.float32),
            pltpu.VMEM((count, 7, 1, width), jnp.float32),
            dma((count, 3)), dma,
            dma((count, 7)), dma((count, 7)),
            dma((count, 2)), dma((count, 2)), dma((count, 2)),
            dma((3,)), dma((3,)),
        ],
        compiler_params=pltpu.CompilerParams(
            collective_id=0, has_side_effects=True,
            vmem_limit_bytes=VMEM_BYTES - 3 * 16 * rows * cols - 2**20,
        ),
        name="gather",
    )(*(
        pltpu.with_memory_space_constraint(a, pltpu.HBM)
        for a in (*args[:9], args[9].reshape(1, rows))
    ))
    ready = jax.ShapeDtypeStruct(big, jnp.bfloat16)
    line = jax.ShapeDtypeStruct((cols,), jnp.float32)
    return pl.pallas_call(
        write_kernel,
        out_shape=[ready] * 3 + [line] * 3,
        in_specs=[vmem] * 4,
        out_specs=[hbm] * 3 + [vmem] * 3,
        scratch_shapes=[dma((3, 4))],
        compiler_params=pltpu.CompilerParams(vmem_limit_bytes=2**20),
        name="write",
    )(*gathered, factor)


def on_device(*args, devices):
    rows, cols = args[0].shape
    total_rows = devices * rows
    fits = rows * cols * (36 + 48) <= 48 * 2**20
    if devices == 8 and rows % 128 == 0 and cols % (128 * UNITS) == 0 and fits:
        return tuple(ringed(*args, total_rows=total_rows))
    return plain(*args, rows=total_rows)


def solution(mesh):
    return jax.shard_map(
        functools.partial(on_device, devices=mesh.shape["fsdp"]),
        mesh=mesh,
        in_specs=(P("fsdp", "model"),) * 9 + (P("fsdp"),),
        out_specs=(P(None, "model"),) * 3 + (P("model"),) * 3,
        check_vma=False,
    )
```
